512 devices in a mesh: trial: 4 (over x), span: 16 (over y, core), heads: 8 (over z).
Axes of the slice: x: 4, y: 8, z: 8, core: 2. Of those that a mesh axis runs over, the one named last changes fastest.
Arguments:
- latents: bfloat16 [64, 4096, 512], P('trial', ('span', 'heads')), parts along dimension 0, may hold values from -6 to 6
- rotary_rows: bfloat16 [64, 4096, 64], P('trial', ('span', 'heads')), parts along dimension 0, may hold values from -6 to 6
- latent_gain: float32 [512], replicated, may hold values from 0.25 to 1.75
- key_up: bfloat16 [2048, 16, 128], P('trial', 'heads'), parts along dimension 0, may hold values from -0.25 to 0.25
- value_up: bfloat16 [2048, 16, 128], P('trial', 'heads'), parts along dimension 0, may hold values from -0.25 to 0.25
Outputs:
- cache_keys: bfloat16 [64, 16, 192, 4096], P(('trial', 'span'), 'heads'), parts along dimension 0
- cache_values: bfloat16 [64, 4096, 16, 128], P(('trial', 'span'), None, 'heads'), parts along dimension 0
The draws below stay inside these ranges and needn't reach their ends.
There are 4 independent parts, one for each index of `trial`. The reference program is written for one: setup_inputs(seed, part) draws one part's arguments, and reference() takes and returns one part's arrays. A program takes and returns all parts, laid end to end along the dimension named above; an argument that names none is the same for every part. Nothing has to cross between parts.
All inputs are finite; a program needn't handle non-finite values.
Results may differ from the reference program's by a relative error of at most 0.0049.
Values may be sent and summed in bfloat16 or wider, within the bound.
A program may use at most 64 MiB of HBM per device.

```python
import jax
import jax.numpy as jnp
from jax import lax

BATCH = 16
LENGTH = 4096
HEADS = 16
LATENT = 512
KEY_PART = 128
ROTARY = 64
VALUE_SIZE = 128


def shard_levels(key, extent, shards, smallest, high):
    level, own = 1.0, jax.random.fold_in(key, 6)
    for dim, blocks in shards:
        steps = jnp.exp(jax.random.uniform(jax.random.fold_in(own, dim), (blocks,), jnp.float32, smallest / len(shards), high / len(shards)))
        level = level * jnp.repeat(steps, extent[dim] // blocks).reshape([-1 if axis == dim else 1 for axis in range(len(extent))])
    return level


def bell_draw(own_key, shape, width, most, cuts=(), kind=jnp.bfloat16):
    values = width * jax.random.normal(own_key, shape, jnp.float32)
    if cuts:
        values = values * shard_levels(own_key, shape, cuts, -0.22, 0.18)
    return jnp.clip(values, -most, most).astype(kind)


def setup_inputs(seed: int = 0, part: int = 0) -> dict:
    seeds = jax.random.split(jax.random.key(seed), 6)
    own_keys = jax.random.split(jax.random.fold_in(seeds[5], part), 6)
    return {
        "latents": bell_draw(own_keys[0], (BATCH, LENGTH, LATENT), 1.0, 6.0, ((1, 128),)),
        "rotary_rows": bell_draw(own_keys[1], (BATCH, LENGTH, ROTARY), 1.0, 6.0, ((1, 128),)),
        "latent_gain": jnp.clip(1.0 + 0.15 * jax.random.normal(seeds[2], (LATENT,), jnp.float32), 0.25, 1.75),
        "key_up": bell_draw(own_keys[3], (LATENT, HEADS, KEY_PART), LATENT ** -0.5, 0.25, ((1, 8),)),
        "value_up": bell_draw(own_keys[4], (LATENT, HEADS, VALUE_SIZE), LATENT ** -0.5, 0.25, ((1, 8),)),
    }


def unit_rows(vectors, row_gain):
    return vectors * lax.rsqrt(lax.optimization_barrier(jnp.mean(vectors * vectors, axis=-1, keepdims=True)) + 1e-06) * row_gain

def reference(latents, rotary_rows, latent_gain, key_up, value_up):
    rows_ready = unit_rows(latents.astype(jnp.float32), latent_gain).astype(jnp.bfloat16)
    rows_ready = lax.optimization_barrier(rows_ready)

    def expand_one(one):
        rows_one, rotary_one = one
        wide_keys = jnp.einsum('tr,rhk->thk', rows_one.astype(jnp.float32), key_up.astype(jnp.float32)).astype(jnp.bfloat16)
        shared = jnp.broadcast_to(rotary_one[:, None], (LENGTH, HEADS, ROTARY))
        wide_values = jnp.einsum('tr,rhk->thk', rows_one.astype(jnp.float32), value_up.astype(jnp.float32)).astype(jnp.bfloat16)
        return (jnp.concatenate([wide_keys, shared], axis=-1), wide_values)
    cache_keys, cache_values = lax.map(expand_one, (rows_ready, rotary_rows))
    cache_keys = jnp.transpose(cache_keys, (0, 2, 3, 1))
    return (cache_keys, cache_values)
```

```python
import jax
import jax.numpy as jnp
from jax import lax
from jax.experimental import pallas as pl
from jax.experimental.pallas import tpu as pltpu
from jax.sharding import PartitionSpec as P

MESH = pl.DeviceIdType.MESH
SPAN = 16
RING = 8
ROWS = 32
LATENT = 512
ROTARY = 64
PART = 128
CHUNK = 144
GROUP = 4
TILE = RING * ROWS


def source_of(j, span):
    i = j // 2
    odd = i % 2
    dy = odd * ((i + 1) // 2) + (1 - odd) * (8 - i // 2)
    y, core = span // 2, span % 2
    swap = j % 2
    other = core + swap - 2 * core * swap
    return ((y + dy) % 8) * 2 + other


def target_of(j, span):
    i = j // 2
    odd = i % 2
    dy = odd * ((i + 1) // 2) + (1 - odd) * (8 - i // 2)
    y, core = span // 2, span % 2
    swap = j % 2
    other = core + swap - 2 * core * swap
    return ((y + 8 - dy) % 8) * 2 + other


def kernel(
    lat_hbm, rot_hbm, gain_hbm, wk_hbm, wv_hbm,
    keys_hbm, values_hbm,
    lat, rot, gain, wk_pairs, wv_pairs, wide, wk, wv,
    ready, held, kst, vwide, vst,
    in_sem, swap_send, swap_recv, up_send, up_recv, down_send, down_recv, out_sem,
):
    span, z = lax.axis_index("span"), lax.axis_index("heads")
    up, down = (z + 1) % RING, (z + RING - 1) % RING

    barrier = pltpu.get_barrier_semaphore()
    for j in range(1, SPAN):
        pl.semaphore_signal(barrier, inc=1, device_id={"span": target_of(j, span)}, device_id_type=MESH)
    for peer in (up, down):
        pl.semaphore_signal(barrier, inc=1, device_id={"heads": peer}, device_id_type=MESH)

    loads = [
        pltpu.make_async_copy(src, dst, in_sem.at[n])
        for n, (src, dst) in enumerate(
            ((lat_hbm, lat), (gain_hbm, gain), (rot_hbm, rot), (wk_hbm, wk_pairs), (wv_hbm, wv_pairs))
        )
    ]
    for load in loads:
        load.start()
    for load in loads[:3]:
        load.wait()

    def make_ready(s, carry):
        x = lat[s].astype(jnp.float32)
        x = x * lax.rsqrt(jnp.mean(x * x, axis=-1, keepdims=True) + 1e-06) * gain[...]
        x = x.astype(jnp.bfloat16)
        for q in range(4):
            ready[s, pl.ds(q * ROWS, ROWS), :] = x[:, q * 128 : (q + 1) * 128]
        r = rot[s]
        ready[s, pl.ds(4 * ROWS, 16), :] = jnp.concatenate([r[:16], r[16:]], axis=1)
        return carry

    lax.fori_loop(0, SPAN, make_ready, 0, unroll=4)
    held[0, z] = ready[span]

    pl.semaphore_wait(barrier, SPAN - 1 + 2)

    def swap(j):
        target = target_of(j, span)
        return pltpu.make_async_remote_copy(
            src_ref=ready.at[target],
            dst_ref=held.at[j, z],
            send_sem=swap_send,
            recv_sem=swap_recv.at[j],
            device_id={"span": target},
            device_id_type=MESH,
        )

    def upward(j, k):
        owner = (z + RING - k) % RING
        return pltpu.make_async_remote_copy(
            src_ref=held.at[j, owner],
            dst_ref=held.at[j, owner],
            send_sem=up_send,
            recv_sem=up_recv.at[j, k],
            device_id={"heads": up},
            device_id_type=MESH,
        )

    def downward(j, k):
        owner = (z + k) % RING
        return pltpu.make_async_remote_copy(
            src_ref=held.at[j, owner],
            dst_ref=held.at[j, owner],
            send_sem=down_send,
            recv_sem=down_recv.at[j, k],
            device_id={"heads": down},
            device_id_type=MESH,
        )

    def send_step(g, k):
        for m in range(GROUP):
            j = g * GROUP + m
            if k == 0:
                @pl.when(j > 0)
                def _():
                    swap(j).wait_recv()
            if k < 3 or m < 2:
                if k > 0:
                    upward(j, k - 1).wait_recv()
                upward(j, k).start()
            if k < 3 or m >= 2:
                if k > 0:
                    downward(j, k - 1).wait_recv()
                downward(j, k).start()

    def finish(g, m):
        j = g * GROUP + m
        upward(j, 3 if m < 2 else 2).wait_recv()
        downward(j, 2 if m < 2 else 3).wait_recv()
        rows = jnp.concatenate(
            [held[j, :, pl.ds(q * ROWS, ROWS), :].reshape(TILE, 128) for q in range(4)], axis=1
        )
        keys = lax.dot_general(
            wk[...], rows, (((1,), (1,)), ((), ())), preferred_element_type=jnp.float32
        ).astype(jnp.bfloat16)
        turned = held[j, :, pl.ds(4 * ROWS, 16), :].astype(jnp.float32)
        turned = jnp.concatenate([turned[:, :, :ROTARY], turned[:, :, ROTARY:]], axis=1)
        turned = turned.reshape(TILE, ROTARY).T.astype(jnp.bfloat16)
        values = jnp.dot(rows, wv[...], preferred_element_type=jnp.float32)
        for h in range(2):
            kst[j, h, pl.ds(0, PART), :] = keys[h * PART : (h + 1) * PART]
            kst[j, h, pl.ds(PART, ROTARY), :] = turned
            vwide[pl.ds(h, TILE, stride=2), :] = values[:, h * PART : (h + 1) * PART]
        vst[j] = vwide[...].astype(jnp.bfloat16)
        source = source_of(j, span)
        pltpu.make_async_copy(
            kst.at[j], keys_hbm.at[:, :, pl.ds(pl.multiple_of(source * TILE, TILE), TILE)], out_sem.at[0]
        ).start()
        pltpu.make_async_copy(
            vst.at[j], values_hbm.at[pl.ds(pl.multiple_of(source * 2 * TILE, 2 * TILE), 2 * TILE), :], out_sem.at[1]
        ).start()

    for j in range(1, SPAN):
        swap(j).start()

    for load in loads[3:]:
        load.wait()
    wide[...] = wk_pairs[...].astype(jnp.float32)
    for h in range(2):
        wk[pl.ds(h * PART, PART), :] = wide[pl.ds(h, LATENT, stride=2), :].T.astype(jnp.bfloat16)
    wide[...] = wv_pairs[...].astype(jnp.float32)
    for h in range(2):
        wv[:, pl.ds(h * PART, PART)] = wide[pl.ds(h, LATENT, stride=2), :].astype(jnp.bfloat16)

    def group(g, carry):
        send_step(g, 0)
        send_step(g, 1)

        @pl.when(g > 0)
        def _():
            finish(g - 1, 0)
            finish(g - 1, 1)

        send_step(g, 2)

        @pl.when(g > 0)
        def _():
            finish(g - 1, 2)
            finish(g - 1, 3)

        send_step(g, 3)
        return carry

    lax.fori_loop(0, SPAN // GROUP, group, 0)
    for m in (0, 2, 1, 3):
        finish(SPAN // GROUP - 1, m)

    def all_of(ref, sem):
        pltpu.make_async_copy(ref, ref, sem).wait()

    all_of(ready.at[pl.ds(0, SPAN - 1)], swap_send)
    all_of(held.at[pl.ds(0, 7)], up_send)
    all_of(held.at[pl.ds(0, 7)], down_send)
    all_of(kst, out_sem.at[0])
    all_of(vst, out_sem.at[1])


def shards(latents, rotary_rows, latent_gain, key_up, value_up):
    anywhere = pl.BlockSpec(memory_space=pl.ANY)
    keys, values = pl.pallas_call(
        kernel,
        out_shape=(
            jax.ShapeDtypeStruct((2, PART + ROTARY, SPAN * TILE), jnp.bfloat16),
            jax.ShapeDtypeStruct((SPAN * TILE * 2, PART), jnp.bfloat16),
        ),
        in_specs=[anywhere] * 5,
        out_specs=(anywhere, anywhere),
        scratch_shapes=[
            pltpu.VMEM((SPAN, ROWS, LATENT), jnp.bfloat16),
            pltpu.VMEM((SPAN, ROWS, ROTARY), jnp.bfloat16),
            pltpu.VMEM((1, LATENT), jnp.float32),
            pltpu.VMEM((2 * LATENT, PART), jnp.bfloat16),
            pltpu.VMEM((2 * LATENT, PART), jnp.bfloat16),
            pltpu.VMEM((2 * LATENT, PART), jnp.float32),
            pltpu.VMEM((2 * PART, LATENT), jnp.bfloat16),
            pltpu.VMEM((LATENT, 2 * PART), jnp.bfloat16),
            pltpu.VMEM((SPAN, CHUNK, 128), jnp.bfloat16),
            pltpu.VMEM((SPAN, RING, CHUNK, 128), jnp.bfloat16),
            pltpu.VMEM((SPAN, 2, PART + ROTARY, TILE), jnp.bfloat16),
            pltpu.VMEM((2 * TILE, PART), jnp.float32),
            pltpu.VMEM((SPAN, 2 * TILE, PART), jnp.bfloat16),
            pltpu.SemaphoreType.DMA((5,)),
            pltpu.SemaphoreType.DMA,
            pltpu.SemaphoreType.DMA((SPAN,)),
            pltpu.SemaphoreType.DMA,
            pltpu.SemaphoreType.DMA((SPAN, 4)),
            pltpu.SemaphoreType.DMA,
            pltpu.SemaphoreType.DMA((SPAN, 4)),
            pltpu.SemaphoreType.DMA((2,)),
        ],
        compiler_params=pltpu.CompilerParams(collective_id=0, has_side_effects=True),
    )(
        latents,
        rotary_rows,
        latent_gain.reshape(1, LATENT),
        key_up.reshape(2 * LATENT, PART),
        value_up.reshape(2 * LATENT, PART),
    )
    return keys[None], values.reshape(1, SPAN * TILE, 2, PART)


def solution(mesh):
    return jax.shard_map(
        shards,
        mesh=mesh,
        in_specs=(
            P("trial", ("span", "heads"), None),
            P("trial", ("span", "heads"), None),
            P(),
            P("trial", "heads", None),
            P("trial", "heads", None),
        ),
        out_specs=(
            P(("trial", "span"), "heads", None, None),
            P(("trial", "span"), None, "heads", None),
        ),
        check_vma=False,
    )
```

```python
import jax
import jax.numpy as jnp
from jax import lax
from jax.experimental import pallas as pl
from jax.experimental.pallas import tpu as pltpu
from jax.sharding import PartitionSpec as P

MESH = pl.DeviceIdType.MESH
SPAN = 16
RING = 8
ROWS = 32
LATENT = 512
ROTARY = 64
PART = 128
CHUNK = 144
GROUP = 8
TILE = RING * ROWS


def source_of(j, span):
    i = j // 2
    odd = i % 2
    dy = odd * ((i + 1) // 2) + (1 - odd) * (8 - i // 2)
    y, core = span // 2, span % 2
    swap = j % 2
    other = core + swap - 2 * core * swap
    return ((y + dy) % 8) * 2 + other


def target_of(j, span):
    i = j // 2
    odd = i % 2
    dy = odd * ((i + 1) // 2) + (1 - odd) * (8 - i // 2)
    y, core = span // 2, span % 2
    swap = j % 2
    other = core + swap - 2 * core * swap
    return ((y + 8 - dy) % 8) * 2 + other


def schedule():
    half = GROUP // 2
    order = [m // 2 + half * (m % 2) for m in range(GROUP)]
    events, owed = [], []
    for first in range(0, SPAN, GROUP):
        for step in range(4):
            for m in range(GROUP):
                if step < 3 or m < half:
                    events.append(("up", first + m, step))
                if step < 3 or m >= half:
                    events.append(("down", first + m, step))
            events += [("finish", j, 0) for j in owed[:half]]
            owed = owed[half:]
        owed = [first + m for m in order]
    return events + [("finish", j, 0) for j in owed]


def gather_kernel(
    lat_hbm, rot_hbm, gain_hbm, wk_hbm, wv_hbm,
    kst, vst,
    own_lat, lat, rot, gain, wk_pairs, wv_pairs, wide, wk, wv, ready, held, vwide,
    in_sem, swap_send, swap_recv, up_send, up_recv, down_send, down_recv,
):
    span, z = lax.axis_index("span"), lax.axis_index("heads")
    up, down = (z + 1) % RING, (z + RING - 1) % RING
    half = GROUP // 2

    barrier = pltpu.get_barrier_semaphore()
    for peer in (up, down):
        pl.semaphore_signal(barrier, inc=1, device_id={"heads": peer}, device_id_type=MESH)
    for j in range(1, SPAN):
        pl.semaphore_signal(barrier, inc=1, device_id={"span": target_of(j, span)}, device_id_type=MESH)

    loads = [
        pltpu.make_async_copy(source, into, in_sem.at[n])
        for n, (source, into) in enumerate(
            (
                (lat_hbm.at[span], own_lat), (gain_hbm, gain), (rot_hbm, rot),
                (lat_hbm, lat), (wk_hbm, wk_pairs), (wv_hbm, wv_pairs),
            )
        )
    ]
    for load in loads:
        load.start()

    def packed(x, r, store):
        x = x.astype(jnp.float32)
        x = x * lax.rsqrt(jnp.mean(x * x, axis=-1, keepdims=True) + 1e-06) * gain[...]
        x = x.astype(jnp.bfloat16)
        for q in range(4):
            store(pl.ds(q * ROWS, ROWS), x[:, q * 128 : (q + 1) * 128])
        store(pl.ds(4 * ROWS, 16), jnp.concatenate([r[:16], r[16:]], axis=1))

    def swap(j):
        return pltpu.make_async_remote_copy(
            src_ref=ready.at[j],
            dst_ref=held.at[j, z],
            send_sem=swap_send,
            recv_sem=swap_recv.at[j],
            device_id={"span": target_of(j, span)},
            device_id_type=MESH,
        )

    def hop(way, j, k):
        owner = (z + RING - k) % RING if way == "up" else (z + k) % RING
        return pltpu.make_async_remote_copy(
            src_ref=held.at[j, owner],
            dst_ref=held.at[j, owner],
            send_sem=up_send if way == "up" else down_send,
            recv_sem=(up_recv if way == "up" else down_recv).at[j, k],
            device_id={"heads": up if way == "up" else down},
            device_id_type=MESH,
        )

    def finish(j):
        rows = jnp.concatenate(
            [held[j, :, pl.ds(q * ROWS, ROWS), :].reshape(TILE, 128) for q in range(4)], axis=1
        )
        keys = lax.dot_general(
            wk[...], rows, (((1,), (1,)), ((), ())), preferred_element_type=jnp.float32
        ).astype(jnp.bfloat16)
        turned = held[j, :, pl.ds(4 * ROWS, 16), :].astype(jnp.float32)
        turned = jnp.concatenate([turned[:, :, :ROTARY], turned[:, :, ROTARY:]], axis=1)
        turned = turned.reshape(TILE, ROTARY).T.astype(jnp.bfloat16)
        values = jnp.dot(rows, wv[...], preferred_element_type=jnp.float32)
        for h in range(2):
            kst[j, h, pl.ds(0, PART), :] = keys[h * PART : (h + 1) * PART]
            kst[j, h, pl.ds(PART, ROTARY), :] = turned
            vwide[pl.ds(h, TILE, stride=2), :] = values[:, h * PART : (h + 1) * PART]
        vst[j] = vwide[...].astype(jnp.bfloat16)

    def store_own(at, x):
        held[0, z, at, :] = x

    def prepare(j):
        target = target_of(j, span)

        def store(at, x):
            ready[j, at, :] = x

        packed(lat[target], rot[target], store)

    for load in loads[:3]:
        load.wait()
    packed(own_lat[...], rot[span], store_own)
    loads[3].wait()
    prepare(1)
    pl.semaphore_wait(barrier, SPAN - 1 + 2)
    hop("up", 0, 0).start()
    hop("down", 0, 0).start()
    for j in range(1, SPAN):
        if j + 1 < SPAN:
            prepare(j + 1)
        swap(j).start()

    arrived = set()

    def arrive(kind, j, k):
        if (kind, j, k) not in arrived:
            arrived.add((kind, j, k))
            if kind == "swap":
                swap(j).wait_recv()
            else:
                hop(kind, j, k).wait_recv()

    weighed = False
    for kind, j, k in schedule():
        if kind == "finish":
            if not weighed:
                weighed = True
                for load in loads[4:]:
                    load.wait()
                wide[...] = wk_pairs[...].astype(jnp.float32)
                for h in range(2):
                    wk[pl.ds(h * PART, PART), :] = wide[pl.ds(h, LATENT, stride=2), :].T.astype(jnp.bfloat16)
                wide[...] = wv_pairs[...].astype(jnp.float32)
                for h in range(2):
                    wv[:, pl.ds(h * PART, PART)] = wide[pl.ds(h, LATENT, stride=2), :].astype(jnp.bfloat16)
            last_up = 3 if j % GROUP < half else 2
            arrive("up", j, last_up)
            arrive("down", j, 5 - last_up)
            finish(j)
        elif (j, k) != (0, 0):
            if k > 0:
                arrive(kind, j, k - 1)
            else:
                arrive("swap", j, 0)
            hop(kind, j, k).start()

    def all_of(ref, sem):
        pltpu.make_async_copy(ref, ref, sem).wait()

    all_of(ready.at[pl.ds(1, SPAN - 1)], swap_send)
    all_of(held.at[pl.ds(0, 7)], up_send)
    all_of(held.at[pl.ds(0, 7)], down_send)


def write_kernel(kst, vst, keys_hbm, values_hbm, sem):
    span = lax.axis_index("span")
    for j in range(SPAN):
        at = source_of(j, span) * TILE
        pltpu.make_async_copy(kst.at[j], keys_hbm.at[:, :, pl.ds(pl.multiple_of(at, TILE), TILE)], sem.at[0]).start()
        pltpu.make_async_copy(
            vst.at[j], values_hbm.at[pl.ds(pl.multiple_of(2 * at, 2 * TILE), 2 * TILE), :], sem.at[1]
        ).start()
    pltpu.make_async_copy(kst, kst, sem.at[0]).wait()
    pltpu.make_async_copy(vst, vst, sem.at[1]).wait()


def shards(latents, rotary_rows, latent_gain, key_up, value_up):
    anywhere = pl.BlockSpec(memory_space=pl.ANY)
    here = pl.BlockSpec(memory_space=pltpu.VMEM)
    kst, vst = pl.pallas_call(
        gather_kernel,
        out_shape=(
            pltpu.VMEM((SPAN, 2, PART + ROTARY, TILE), jnp.bfloat16),
            pltpu.VMEM((SPAN, 2 * TILE, PART), jnp.bfloat16),
        ),
        in_specs=[pl.BlockSpec(memory_space=pltpu.HBM)] * 5,
        out_specs=(here, here),
        scratch_shapes=[
            pltpu.VMEM((ROWS, LATENT), jnp.bfloat16),
            pltpu.VMEM((SPAN, ROWS, LATENT), jnp.bfloat16),
            pltpu.VMEM((SPAN, ROWS, ROTARY), jnp.bfloat16),
            pltpu.VMEM((1, LATENT), jnp.float32),
            pltpu.VMEM((2 * LATENT, PART), jnp.bfloat16),
            pltpu.VMEM((2 * LATENT, PART), jnp.bfloat16),
            pltpu.VMEM((2 * LATENT, PART), jnp.float32),
            pltpu.VMEM((2 * PART, LATENT), jnp.bfloat16),
            pltpu.VMEM((LATENT, 2 * PART), jnp.bfloat16),
            pltpu.VMEM((SPAN, CHUNK, 128), jnp.bfloat16),
            pltpu.VMEM((SPAN, RING, CHUNK, 128), jnp.bfloat16),
            pltpu.VMEM((2 * TILE, PART), jnp.float32),
            pltpu.SemaphoreType.DMA((6,)),
            pltpu.SemaphoreType.DMA,
            pltpu.SemaphoreType.DMA((SPAN,)),
            pltpu.SemaphoreType.DMA,
            pltpu.SemaphoreType.DMA((SPAN, 4)),
            pltpu.SemaphoreType.DMA,
            pltpu.SemaphoreType.DMA((SPAN, 4)),
        ],
        compiler_params=pltpu.CompilerParams(
            collective_id=0, has_side_effects=True, vmem_limit_bytes=24 * 2**20
        ),
    )(
        *(
            pltpu.with_memory_space_constraint(x, pltpu.HBM)
            for x in (
                latents,
                rotary_rows,
                latent_gain.reshape(1, LATENT),
                key_up.reshape(2 * LATENT, PART),
                value_up.reshape(2 * LATENT, PART),
            )
        )
    )
    keys, values = pl.pallas_call(
        write_kernel,
        out_shape=(
            jax.ShapeDtypeStruct((2, PART + ROTARY, SPAN * TILE), jnp.bfloat16),
            jax.ShapeDtypeStruct((SPAN * TILE * 2, PART), jnp.bfloat16),
        ),
        in_specs=[anywhere, anywhere],
        out_specs=(anywhere, anywhere),
        scratch_shapes=[pltpu.SemaphoreType.DMA((2,))],
        compiler_params=pltpu.CompilerParams(vmem_limit_bytes=24 * 2**20),
    )(kst, vst)
    return keys[None], values.reshape(1, SPAN * TILE, 2, PART)


def solution(mesh):
    return jax.shard_map(
        shards,
        mesh=mesh,
        in_specs=(
            P("trial", ("span", "heads"), None),
            P("trial", ("span", "heads"), None),
            P(),
            P("trial", "heads", None),
            P("trial", "heads", None),
        ),
        out_specs=(
            P(("trial", "span"), "heads", None, None),
            P(("trial", "span"), None, "heads", None),
        ),
        check_vma=False,
    )
```

```python
import jax
import jax.numpy as jnp
from jax import lax
from jax.experimental import pallas as pl
from jax.experimental.pallas import tpu as pltpu
from jax.sharding import PartitionSpec as P

MESH = pl.DeviceIdType.MESH
SPAN = 16
RING = 8
ROWS = 32
LATENT = 512
ROTARY = 64
PART = 128
CHUNK = 144
MOVED = 4
WEIGH_AT = 40
TILE = RING * ROWS


def source_of(j, span):
    i = j // 2
    odd = i % 2
    dy = odd * ((i + 1) // 2) + (1 - odd) * (8 - i // 2)
    y, core = span // 2, span % 2
    swap = j % 2
    other = core + swap - 2 * core * swap
    return ((y + dy) % 8) * 2 + other


def target_of(j, span):
    i = j // 2
    odd = i % 2
    dy = odd * ((i + 1) // 2) + (1 - odd) * (8 - i // 2)
    y, core = span // 2, span % 2
    swap = j % 2
    other = core + swap - 2 * core * swap
    return ((y + 8 - dy) % 8) * 2 + other


KINDS = ("up", "down", "finish")
ORDER = (
    68, 4, 72, 8, 65, 1, 76, 12, 80, 16, 84, 20, 69, 5, 88, 24, 73, 9, 92, 28, 66, 2, 77, 13, 96, 32, 81, 17,
    100, 36, 85, 21, 104, 40, 89, 25, 108, 44, 93, 29, 112, 48, 97, 33, 116, 52, 101, 37, 120, 56, 105, 41,
    124, 60, 109, 45, 70, 6, 113, 49, 74, 10, 117, 53, 78, 14, 121, 57, 82, 18, 125, 61, 86, 22, 90, 26, 94,
    30, 98, 34, 102, 38, 106, 42, 110, 46, 114, 50, 118, 54, 122, 58, 126, 62, 99, 3, 83, 103, 7, 87, 107, 11,
    91, 111, 15, 95, 115, 19, 119, 23, 123, 27, 127, 31, 128, 132, 136, 140, 144, 148, 152, 156,
)


def schedule():
    return [(KINDS[code // 64], code // 4 % 16, code % 4) for code in ORDER]


def gather_kernel(
    lat_hbm, rot_hbm, gain_hbm, wk_hbm, wv_hbm,
    kst, vst,
    own_lat, lat, rot, gain, wk_pairs, wv_pairs, wide, wk, wv, ready, held, vwide,
    in_sem, swap_send, swap_recv, up_send, up_recv, down_send, down_recv, moved_send, known,
):
    span, z = lax.axis_index("span"), lax.axis_index("heads")
    up, down = (z + 1) % RING, (z + RING - 1) % RING

    loads = [
        pltpu.make_async_copy(source, into, in_sem.at[n])
        for n, (source, into) in enumerate(
            (
                (lat_hbm.at[span], own_lat), (gain_hbm, gain), (rot_hbm, rot),
                (lat_hbm, lat), (wk_hbm, wk_pairs), (wv_hbm, wv_pairs),
            )
        )
    ]
    for load in loads[:3]:
        load.start()

    y, core = span // 2, span % 2
    beside = [2 * ((y + step) % 8) for step in (1, 7)]
    barrier = pltpu.get_barrier_semaphore()
    for peer in (up, down):
        pl.semaphore_signal(barrier, inc=1, device_id={"heads": peer}, device_id_type=MESH)
    for peer in (2 * y + 1 - core, *(first + c for first in beside for c in range(2))):
        pl.semaphore_signal(barrier, inc=1, device_id={"span": peer}, device_id_type=MESH)

    for load in loads[3:]:
        load.start()

    def tell(level):
        for first in beside:
            pl.semaphore_signal(known.at[level], inc=1, device_id={"span": first + core}, device_id_type=MESH)

    def hear(level):
        pl.semaphore_wait(known.at[level], 2)

    def packed(x, r, store):
        x = x.astype(jnp.float32)
        x = x * lax.rsqrt(jnp.mean(x * x, axis=-1, keepdims=True) + 1e-06) * gain[...]
        x = x.astype(jnp.bfloat16)
        for q in range(4):
            store(pl.ds(q * ROWS, ROWS), x[:, q * 128 : (q + 1) * 128])
        store(pl.ds(4 * ROWS, 16), jnp.concatenate([r[:16], r[16:]], axis=1))

    def swap(j):
        return pltpu.make_async_remote_copy(
            src_ref=ready.at[j],
            dst_ref=held.at[j, z],
            send_sem=swap_send,
            recv_sem=swap_recv.at[j],
            device_id={"span": target_of(j, span)},
            device_id_type=MESH,
        )

    def hop(way, j, k, sent=None):
        owner = (z + RING - k) % RING if way == "up" else (z + k) % RING
        return pltpu.make_async_remote_copy(
            src_ref=held.at[j, owner],
            dst_ref=held.at[j, owner],
            send_sem=(up_send if way == "up" else down_send) if sent is None else sent,
            recv_sem=(up_recv if way == "up" else down_recv).at[j, k],
            device_id={"heads": up if way == "up" else down},
            device_id_type=MESH,
        )

    def finish(j):
        rows = jnp.concatenate(
            [held[j, :, pl.ds(q * ROWS, ROWS), :].reshape(TILE, 128) for q in range(4)], axis=1
        )
        keys = lax.dot_general(
            wk[...], rows, (((1,), (1,)), ((), ())), preferred_element_type=jnp.float32
        ).astype(jnp.bfloat16)
        turned = held[j, :, pl.ds(4 * ROWS, 16), :].astype(jnp.float32)
        turned = jnp.concatenate([turned[:, :, :ROTARY], turned[:, :, ROTARY:]], axis=1)
        turned = turned.reshape(TILE, ROTARY).T.astype(jnp.bfloat16)
        values = jnp.dot(rows, wv[...], preferred_element_type=jnp.float32)
        for h in range(2):
            kst[j, h, pl.ds(0, PART), :] = keys[h * PART : (h + 1) * PART]
            kst[j, h, pl.ds(PART, ROTARY), :] = turned
            vwide[pl.ds(h, TILE, stride=2), :] = values[:, h * PART : (h + 1) * PART]
        vst[j] = vwide[...].astype(jnp.bfloat16)

    def store_own(at, x):
        held[0, z, at, :] = x

    def prepare(j):
        target = target_of(j, span)

        def store(at, x):
            ready[j, at, :] = x

        packed(lat[target], rot[target], store)

    for load in loads[:3]:
        load.wait()
    packed(own_lat[...], rot[span], store_own)
    loads[3].wait()
    prepare(1)
    pl.semaphore_wait(barrier, 7)
    tell(0)
    hop("up", 0, 0).start()
    hop("down", 0, 0).start()
    swapped = set()

    def start_swaps(upto):
        for j in range(1, upto + 1):
            if j not in swapped:
                swapped.add(j)
                if j in (6, 10, 14):
                    level = j // 4 - 1
                    hear(level)
                    if level < 2:
                        tell(level + 1)
                if j + 1 < SPAN:
                    prepare(j + 1)
                swap(j).start()

    arrived = set()

    def arrive(kind, j, k):
        if (kind, j, k) not in arrived:
            arrived.add((kind, j, k))
            if kind == "swap":
                swap(j).wait_recv()
            else:
                hop(kind, j, k).wait_recv()

    start_swaps(5)
    def weigh():
        for load in loads[4:]:
            load.wait()
        wide[...] = wk_pairs[...].astype(jnp.float32)
        for h in range(2):
            wk[pl.ds(h * PART, PART), :] = wide[pl.ds(h, LATENT, stride=2), :].T.astype(jnp.bfloat16)
        wide[...] = wv_pairs[...].astype(jnp.float32)
        for h in range(2):
            wv[:, pl.ds(h * PART, PART)] = wide[pl.ds(h, LATENT, stride=2), :].astype(jnp.bfloat16)

    for number, (kind, j, k) in enumerate(schedule()):
        if number == WEIGH_AT:
            weigh()
        if kind == "finish":
            pair = (j, j + SPAN // 2)
            for one in pair:
                by_up = one < SPAN // 2
                if by_up and one >= SPAN // 2 - MOVED:
                    pl.when(z == 0)(hop("down", one, 3).wait_recv)
                    pl.when(z != 0)(hop("up", one, 3).wait_recv)
                else:
                    arrive("up" if by_up else "down", one, 3)
                arrive("down" if by_up else "up", one, 2)
            for one in pair:
                finish(one)
        elif (j, k) != (0, 0):
            if k > 0:
                arrive(kind, j, k - 1)
            else:
                arrive("swap", j, 0)
            if k < 3 or not SPAN // 2 - MOVED <= j < SPAN // 2:
                hop(kind, j, k).start()
            elif kind == "up":
                pl.when(z < RING - 1)(hop(kind, j, k).start)
            else:
                pl.when(z == 1)(hop(kind, j, k, moved_send).start)
            if kind == "down" and k == 0:
                start_swaps(min(SPAN - 1, 5 + 4 * j))

    def all_of(ref, sem):
        pltpu.make_async_copy(ref, ref, sem).wait()

    all_of(ready.at[pl.ds(1, SPAN - 1)], swap_send)
    all_of(held.at[pl.ds(0, 7)], down_send)

    @pl.when(z < RING - 1)
    def _():
        all_of(held.at[pl.ds(0, 7)], up_send)

    @pl.when(z == RING - 1)
    def _():
        all_of(held.at[pl.ds(0, 13), pl.ds(0, 4)], up_send)

    @pl.when(z == 1)
    def _():
        all_of(held.at[0, pl.ds(0, MOVED)], moved_send)


def write_kernel(kst, vst, keys_hbm, values_hbm, sem):
    span = lax.axis_index("span")
    for j in range(SPAN):
        at = source_of(j, span) * TILE
        pltpu.make_async_copy(kst.at[j], keys_hbm.at[:, :, pl.ds(pl.multiple_of(at, TILE), TILE)], sem.at[0]).start()
        pltpu.make_async_copy(
            vst.at[j], values_hbm.at[pl.ds(pl.multiple_of(2 * at, 2 * TILE), 2 * TILE), :], sem.at[1]
        ).start()
    pltpu.make_async_copy(kst, kst, sem.at[0]).wait()
    pltpu.make_async_copy(vst, vst, sem.at[1]).wait()


def shards(latents, rotary_rows, latent_gain, key_up, value_up):
    anywhere = pl.BlockSpec(memory_space=pl.ANY)
    here = pl.BlockSpec(memory_space=pltpu.VMEM)
    kst, vst = pl.pallas_call(
        gather_kernel,
        out_shape=(
            pltpu.VMEM((SPAN, 2, PART + ROTARY, TILE), jnp.bfloat16),
            pltpu.VMEM((SPAN, 2 * TILE, PART), jnp.bfloat16),
        ),
        in_specs=[pl.BlockSpec(memory_space=pltpu.HBM)] * 5,
        out_specs=(here, here),
        scratch_shapes=[
            pltpu.VMEM((ROWS, LATENT), jnp.bfloat16),
            pltpu.VMEM((SPAN, ROWS, LATENT), jnp.bfloat16),
            pltpu.VMEM((SPAN, ROWS, ROTARY), jnp.bfloat16),
            pltpu.VMEM((1, LATENT), jnp.float32),
            pltpu.VMEM((2 * LATENT, PART), jnp.bfloat16),
            pltpu.VMEM((2 * LATENT, PART), jnp.bfloat16),
            pltpu.VMEM((2 * LATENT, PART), jnp.float32),
            pltpu.VMEM((2 * PART, LATENT), jnp.bfloat16),
            pltpu.VMEM((LATENT, 2 * PART), jnp.bfloat16),
            pltpu.VMEM((SPAN, CHUNK, 128), jnp.bfloat16),
            pltpu.VMEM((SPAN, RING, CHUNK, 128), jnp.bfloat16),
            pltpu.VMEM((2 * TILE, PART), jnp.float32),
            pltpu.SemaphoreType.DMA((6,)),
            pltpu.SemaphoreType.DMA,
            pltpu.SemaphoreType.DMA((SPAN,)),
            pltpu.SemaphoreType.DMA,
            pltpu.SemaphoreType.DMA((SPAN, 4)),
            pltpu.SemaphoreType.DMA,
            pltpu.SemaphoreType.DMA((SPAN, 4)),
            pltpu.SemaphoreType.DMA,
            pltpu.SemaphoreType.REGULAR((3,)),
        ],
        compiler_params=pltpu.CompilerParams(
            collective_id=0, has_side_effects=True, vmem_limit_bytes=24 * 2**20
        ),
    )(
        *(
            pltpu.with_memory_space_constraint(x, pltpu.HBM)
            for x in (
                latents,
                rotary_rows,
                latent_gain.reshape(1, LATENT),
                key_up.reshape(2 * LATENT, PART),
                value_up.reshape(2 * LATENT, PART),
            )
        )
    )
    keys, values = pl.pallas_call(
        write_kernel,
        out_shape=(
            jax.ShapeDtypeStruct((2, PART + ROTARY, SPAN * TILE), jnp.bfloat16),
            jax.ShapeDtypeStruct((SPAN * TILE * 2, PART), jnp.bfloat16),
        ),
        in_specs=[anywhere, anywhere],
        out_specs=(anywhere, anywhere),
        scratch_shapes=[pltpu.SemaphoreType.DMA((2,))],
        compiler_params=pltpu.CompilerParams(vmem_limit_bytes=24 * 2**20),
    )(kst, vst)
    return keys[None], values.reshape(1, SPAN * TILE, 2, PART)


def solution(mesh):
    return jax.shard_map(
        shards,
        mesh=mesh,
        in_specs=(
            P("trial", ("span", "heads"), None),
            P("trial", ("span", "heads"), None),
            P(),
            P("trial", "heads", None),
            P("trial", "heads", None),
        ),
        out_specs=(
            P(("trial", "span"), "heads", None, None),
            P(("trial", "span"), None, "heads", None),
        ),
        check_vma=False,
    )
```

```python
import jax
import jax.numpy as jnp
from jax import lax
from jax.experimental import pallas as pl
from jax.experimental.pallas import tpu as pltpu
from jax.sharding import PartitionSpec as P

MESH = pl.DeviceIdType.MESH
SPAN = 16
RING = 8
ROWS = 32
LATENT = 512
ROTARY = 64
PART = 128
CHUNK = 144
LAST = (7, 15)
MOVED = 4
WEIGH_AT = 40
TILE = RING * ROWS


def source_of(j, span):
    i = j // 2
    odd = i % 2
    dy = odd * ((i + 1) // 2) + (1 - odd) * (8 - i // 2)
    y, core = span // 2, span % 2
    swap = j % 2
    other = core + swap - 2 * core * swap
    return ((y + dy) % 8) * 2 + other


def target_of(j, span):
    i = j // 2
    odd = i % 2
    dy = odd * ((i + 1) // 2) + (1 - odd) * (8 - i // 2)
    y, core = span // 2, span % 2
    swap = j % 2
    other = core + swap - 2 * core * swap
    return ((y + 8 - dy) % 8) * 2 + other


KINDS = ("up", "down", "finish")
ORDER = (
    68, 4, 72, 8, 65, 1, 76, 12, 80, 16, 84, 20, 69, 5, 88, 24, 73, 9, 92, 28, 96, 32, 77, 13, 100, 36, 104,
    40, 81, 17, 108, 44, 112, 48, 85, 21, 116, 52, 120, 56, 89, 25, 124, 60, 93, 29, 97, 33, 101, 37, 105, 41,
    109, 45, 113, 49, 117, 53, 121, 57, 125, 61, 66, 2, 70, 6, 74, 10, 78, 14, 82, 18, 86, 22, 90, 26, 94, 30,
    98, 34, 102, 38, 106, 42, 110, 46, 114, 50, 118, 54, 122, 58, 126, 62, 99, 3, 83, 103, 7, 87, 107, 11, 91,
    111, 15, 95, 115, 19, 119, 23, 123, 27, 127, 31, 128, 132, 136, 140, 144, 148, 152, 156,
)


def schedule():
    return [(KINDS[code // 64], code // 4 % 16, code % 4) for code in ORDER]


def expand(chunk, wk, wv, vwide, keys_out, values_out):
    rows = jnp.concatenate(
        [chunk[:, pl.ds(q * ROWS, ROWS), :].reshape(TILE, 128) for q in range(4)], axis=1
    )
    keys = lax.dot_general(
        wk[...], rows, (((1,), (1,)), ((), ())), preferred_element_type=jnp.float32
    ).astype(jnp.bfloat16)
    turned = chunk[:, pl.ds(4 * ROWS, 16), :].astype(jnp.float32)
    turned = jnp.concatenate([turned[:, :, :ROTARY], turned[:, :, ROTARY:]], axis=1)
    turned = turned.reshape(TILE, ROTARY).T.astype(jnp.bfloat16)
    values = jnp.dot(rows, wv[...], preferred_element_type=jnp.float32)
    for h in range(2):
        keys_out[h, pl.ds(0, PART), :] = keys[h * PART : (h + 1) * PART]
        keys_out[h, pl.ds(PART, ROTARY), :] = turned
        vwide[pl.ds(h, TILE, stride=2), :] = values[:, h * PART : (h + 1) * PART]
    values_out[...] = vwide[...].astype(jnp.bfloat16)


def gather_kernel(
    lat_hbm, rot_hbm, gain_hbm, wk_hbm, wv_hbm,
    kst, vst, held, wk, wv,
    own_lat, lat, rot, gain, wk_pairs, wv_pairs, wide, ready, vwide,
    in_sem, swap_send, swap_recv, up_send, up_recv, down_send, down_recv, moved_send, known,
):
    span, z = lax.axis_index("span"), lax.axis_index("heads")
    up, down = (z + 1) % RING, (z + RING - 1) % RING

    loads = [
        pltpu.make_async_copy(source, into, in_sem.at[n])
        for n, (source, into) in enumerate(
            (
                (lat_hbm.at[span], own_lat), (gain_hbm, gain), (rot_hbm, rot),
                (lat_hbm, lat), (wk_hbm, wk_pairs), (wv_hbm, wv_pairs),
            )
        )
    ]
    for load in loads[:3]:
        load.start()

    y, core = span // 2, span % 2
    beside = [2 * ((y + step) % 8) for step in (1, 7)]
    barrier = pltpu.get_barrier_semaphore()
    for peer in (up, down):
        pl.semaphore_signal(barrier, inc=1, device_id={"heads": peer}, device_id_type=MESH)
    for peer in (2 * y + 1 - core, *(first + c for first in beside for c in range(2))):
        pl.semaphore_signal(barrier, inc=1, device_id={"span": peer}, device_id_type=MESH)

    for load in loads[3:]:
        load.start()

    def tell(level):
        for first in beside:
            pl.semaphore_signal(known.at[level], inc=1, device_id={"span": first + core}, device_id_type=MESH)

    def hear(level):
        pl.semaphore_wait(known.at[level], 2)

    def packed(x, r, store):
        x = x.astype(jnp.float32)
        x = x * lax.rsqrt(jnp.mean(x * x, axis=-1, keepdims=True) + 1e-06) * gain[...]
        x = x.astype(jnp.bfloat16)
        for q in range(4):
            store(pl.ds(q * ROWS, ROWS), x[:, q * 128 : (q + 1) * 128])
        store(pl.ds(4 * ROWS, 16), jnp.concatenate([r[:16], r[16:]], axis=1))

    def swap(j):
        return pltpu.make_async_remote_copy(
            src_ref=ready.at[j],
            dst_ref=held.at[j, z],
            send_sem=swap_send,
            recv_sem=swap_recv.at[j],
            device_id={"span": target_of(j, span)},
            device_id_type=MESH,
        )

    def hop(way, j, k, sent=None):
        owner = (z + RING - k) % RING if way == "up" else (z + k) % RING
        return pltpu.make_async_remote_copy(
            src_ref=held.at[j, owner],
            dst_ref=held.at[j, owner],
            send_sem=(up_send if way == "up" else down_send) if sent is None else sent,
            recv_sem=(up_recv if way == "up" else down_recv).at[j, k],
            device_id={"heads": up if way == "up" else down},
            device_id_type=MESH,
        )

    def finish(j):
        expand(held.at[j], wk, wv, vwide, kst.at[j], vst.at[j])

    def store_own(at, x):
        held[0, z, at, :] = x

    def prepare(j):
        target = target_of(j, span)

        def store(at, x):
            ready[j, at, :] = x

        packed(lat[target], rot[target], store)

    for load in loads[:3]:
        load.wait()
    packed(own_lat[...], rot[span], store_own)
    loads[3].wait()
    prepare(1)
    pl.semaphore_wait(barrier, 7)
    tell(0)
    hop("up", 0, 0).start()
    hop("down", 0, 0).start()
    swapped = set()

    def start_swaps(upto):
        for j in range(1, upto + 1):
            if j not in swapped:
                swapped.add(j)
                if j in (6, 10, 14):
                    level = j // 4 - 1
                    hear(level)
                    if level < 2:
                        tell(level + 1)
                if j + 1 < SPAN:
                    prepare(j + 1)
                swap(j).start()

    arrived = set()

    def arrive(kind, j, k):
        if (kind, j, k) not in arrived:
            arrived.add((kind, j, k))
            if kind == "swap":
                swap(j).wait_recv()
            else:
                hop(kind, j, k).wait_recv()

    start_swaps(5)
    def weigh():
        for load in loads[4:]:
            load.wait()
        wide[...] = wk_pairs[...].astype(jnp.float32)
        for h in range(2):
            wk[pl.ds(h * PART, PART), :] = wide[pl.ds(h, LATENT, stride=2), :].T.astype(jnp.bfloat16)
        wide[...] = wv_pairs[...].astype(jnp.float32)
        for h in range(2):
            wv[:, pl.ds(h * PART, PART)] = wide[pl.ds(h, LATENT, stride=2), :].astype(jnp.bfloat16)

    for number, (kind, j, k) in enumerate(schedule()):
        if number == WEIGH_AT:
            weigh()
        if kind == "finish":
            pair = (j, j + SPAN // 2)
            for one in pair:
                by_up = one < SPAN // 2
                if by_up and one >= SPAN // 2 - MOVED:
                    pl.when(z == 0)(hop("down", one, 3).wait_recv)
                    pl.when(z != 0)(hop("up", one, 3).wait_recv)
                else:
                    arrive("up" if by_up else "down", one, 3)
                arrive("down" if by_up else "up", one, 2)
            if pair != LAST:
                for one in pair:
                    finish(one)
        elif (j, k) != (0, 0):
            if k > 0:
                arrive(kind, j, k - 1)
            else:
                arrive("swap", j, 0)
            if k < 3 or not SPAN // 2 - MOVED <= j < SPAN // 2:
                hop(kind, j, k).start()
            elif kind == "up":
                pl.when(z < RING - 1)(hop(kind, j, k).start)
            else:
                pl.when(z == 1)(hop(kind, j, k, moved_send).start)
            if kind == "down" and k == 0:
                start_swaps(min(SPAN - 1, 5 + 4 * j))

    def all_of(ref, sem):
        pltpu.make_async_copy(ref, ref, sem).wait()

    all_of(ready.at[pl.ds(1, SPAN - 1)], swap_send)
    all_of(held.at[pl.ds(0, 7)], down_send)

    @pl.when(z < RING - 1)
    def _():
        all_of(held.at[pl.ds(0, 7)], up_send)

    @pl.when(z == RING - 1)
    def _():
        all_of(held.at[pl.ds(0, 13), pl.ds(0, 4)], up_send)

    @pl.when(z == 1)
    def _():
        all_of(held.at[0, pl.ds(0, MOVED)], moved_send)


def write_kernel(kst, vst, held, wk, wv, keys_hbm, values_hbm, vwide, last_keys, last_values, sem):
    span = lax.axis_index("span")

    def write(j, keys, values):
        at = source_of(j, span) * TILE
        pltpu.make_async_copy(keys, keys_hbm.at[:, :, pl.ds(pl.multiple_of(at, TILE), TILE)], sem.at[0]).start()
        pltpu.make_async_copy(
            values, values_hbm.at[pl.ds(pl.multiple_of(2 * at, 2 * TILE), 2 * TILE), :], sem.at[1]
        ).start()

    for j in range(SPAN):
        if j not in LAST:
            write(j, kst.at[j], vst.at[j])
    for n, j in enumerate(LAST):
        expand(held.at[j], wk, wv, vwide.at[n], last_keys.at[n], last_values.at[n])
    for n, j in enumerate(LAST):
        write(j, last_keys.at[n], last_values.at[n])
    pltpu.make_async_copy(kst, kst, sem.at[0]).wait()
    pltpu.make_async_copy(vst, vst, sem.at[1]).wait()


def shards(latents, rotary_rows, latent_gain, key_up, value_up):
    anywhere = pl.BlockSpec(memory_space=pl.ANY)
    here = pl.BlockSpec(memory_space=pltpu.VMEM)
    gathered = pl.pallas_call(
        gather_kernel,
        out_shape=(
            pltpu.VMEM((SPAN, 2, PART + ROTARY, TILE), jnp.bfloat16),
            pltpu.VMEM((SPAN, 2 * TILE, PART), jnp.bfloat16),
            pltpu.VMEM((SPAN, RING, CHUNK, 128), jnp.bfloat16),
            pltpu.VMEM((2 * PART, LATENT), jnp.bfloat16),
            pltpu.VMEM((LATENT, 2 * PART), jnp.bfloat16),
        ),
        in_specs=[pl.BlockSpec(memory_space=pltpu.HBM)] * 5,
        out_specs=(here,) * 5,
        scratch_shapes=[
            pltpu.VMEM((ROWS, LATENT), jnp.bfloat16),
            pltpu.VMEM((SPAN, ROWS, LATENT), jnp.bfloat16),
            pltpu.VMEM((SPAN, ROWS, ROTARY), jnp.bfloat16),
            pltpu.VMEM((1, LATENT), jnp.float32),
            pltpu.VMEM((2 * LATENT, PART), jnp.bfloat16),
            pltpu.VMEM((2 * LATENT, PART), jnp.bfloat16),
            pltpu.VMEM((2 * LATENT, PART), jnp.float32),
            pltpu.VMEM((SPAN, CHUNK, 128), jnp.bfloat16),
            pltpu.VMEM((2 * TILE, PART), jnp.float32),
            pltpu.SemaphoreType.DMA((6,)),
            pltpu.SemaphoreType.DMA,
            pltpu.SemaphoreType.DMA((SPAN,)),
            pltpu.SemaphoreType.DMA,
            pltpu.SemaphoreType.DMA((SPAN, 4)),
            pltpu.SemaphoreType.DMA,
            pltpu.SemaphoreType.DMA((SPAN, 4)),
            pltpu.SemaphoreType.DMA,
            pltpu.SemaphoreType.REGULAR((3,)),
        ],
        compiler_params=pltpu.CompilerParams(
            collective_id=0, has_side_effects=True, vmem_limit_bytes=24 * 2**20
        ),
    )(
        *(
            pltpu.with_memory_space_constraint(x, pltpu.HBM)
            for x in (
                latents,
                rotary_rows,
                latent_gain.reshape(1, LATENT),
                key_up.reshape(2 * LATENT, PART),
                value_up.reshape(2 * LATENT, PART),
            )
        )
    )
    keys, values = pl.pallas_call(
        write_kernel,
        out_shape=(
            jax.ShapeDtypeStruct((2, PART + ROTARY, SPAN * TILE), jnp.bfloat16),
            jax.ShapeDtypeStruct((SPAN * TILE * 2, PART), jnp.bfloat16),
        ),
        in_specs=[here] * 5,
        out_specs=(anywhere, anywhere),
        scratch_shapes=[
            pltpu.VMEM((2, 2 * TILE, PART), jnp.float32),
            pltpu.VMEM((2, 2, PART + ROTARY, TILE), jnp.bfloat16),
            pltpu.VMEM((2, 2 * TILE, PART), jnp.bfloat16),
            pltpu.SemaphoreType.DMA((2,)),
        ],
        compiler_params=pltpu.CompilerParams(vmem_limit_bytes=24 * 2**20),
    )(*(pltpu.with_memory_space_constraint(x, pltpu.VMEM) for x in gathered))
    return keys[None], values.reshape(1, SPAN * TILE, 2, PART)


def solution(mesh):
    return jax.shard_map(
        shards,
        mesh=mesh,
        in_specs=(
            P("trial", ("span", "heads"), None),
            P("trial", ("span", "heads"), None),
            P(),
            P("trial", "heads", None),
            P("trial", "heads", None),
        ),
        out_specs=(
            P(("trial", "span"), "heads", None, None),
            P(("trial", "span"), None, "heads", None),
        ),
        check_vma=False,
    )
```
